32 devices in a mesh: sub: 8 (over z, y), slab: 4 (over x, core).
Axes of the slice: x: 2, y: 2, z: 4, core: 2. Of those that a mesh axis runs over, the one named last changes fastest.
Arguments:
- rhs: float32 [8, 64, 8, 512], P(None, 'sub', None, 'slab'), may hold values from -60 to 60, as said below
- perm: float32 [64, 8, 512], P('sub', None, 'slab'), may hold values from 0.1 to 10
- accum: float32 [64, 8, 512], P('sub', None, 'slab'), may hold values from 0.05 to 0.5
- counts: int32 [8], replicated, may hold values from 1 to 8, as said below
Outputs:
- solution: float32 [8, 64, 8, 512], P(None, 'sub', None, 'slab')
- residual: float32 [8, 64, 8, 512], P(None, 'sub', None, 'slab')
The draws below stay inside these ranges and needn't reach their ends.
Inputs may be any that keep to these rules, and one draw needn't show every extreme that they name: `rhs`: pressure sources of the 8 systems; values on planes that are not live are never read. counts[i] live planes fill the first slots of subdomain i; some subdomain has 8.
All inputs are finite; a program needn't handle non-finite values.
Results may differ from the reference program's by a relative error of at most 0.00045.
Values sent between devices are 32-bit elements; how exact they have to be, the bound alone decides.
A program may use at most 64 MiB of HBM per device.

```python
import math
import jax
import jax.numpy as jnp
from jax import lax

CX = 8
CY = 8
S = 8
ITERS = 4
DEG = 4
NXB = 64
NZ = 512
N_SUB = 8


def draw_rhs(key, part):
    shape = (S, NXB, CY, NZ)
    column = 10.0 ** (jnp.arange(S, dtype=jnp.float32) / (S - 1) - 0.5)
    along = 1.0 + 2.0 * jnp.arange(NXB, dtype=jnp.float32) / (NXB - 1)
    noise = jnp.clip(jax.random.normal(key, shape, jnp.float32), -6.0, 6.0)
    return noise * column[:, None, None, None] * along[None, :, None, None]


def draw_counts(key, part):
    first = jax.random.fold_in(key, 11)
    second = jax.random.fold_in(key, 12)
    counts = jax.random.randint(first, (NXB // CX,), 1, CX + 1)
    full = jax.random.randint(second, (), 0, NXB // CX)
    return counts.at[full].set(CX).astype(jnp.int32)


def shard_levels(rng, shape, shards, smallest, largest):
    loudness = 1.0
    for axis_at, parts in shards:
        draws = jax.random.uniform(jax.random.fold_in(jax.random.fold_in(rng, 6), axis_at), (parts,), jnp.float32, smallest / len(shards), largest / len(shards))
        loudness = loudness * jnp.repeat(jnp.exp(draws), shape[axis_at] // parts).reshape((-1,) + (1,) * (len(shape) - 1 - axis_at))
    return loudness


def setup_inputs(seed: int = 0) -> dict:
    streams_of = jax.random.split(jax.random.key(seed), 5)
    return {
        "rhs": draw_rhs(jax.random.fold_in(streams_of[4], 71), 0),
        "perm": jnp.clip(jnp.exp(math.log(10.0) - 4.6051702 * jax.random.uniform(streams_of[1], (NXB, CY, NZ), jnp.float32) ** shard_levels(streams_of[1], (NXB, CY, NZ), ((0, 8), (2, 4)), -0.2, 0.2)), 0.1, 10.0),
        "accum": jnp.clip(jnp.exp(math.log(0.5) - 2.3025851 * jax.random.uniform(streams_of[2], (NXB, CY, NZ), jnp.float32) ** shard_levels(streams_of[2], (NXB, CY, NZ), ((0, 8), (2, 4)), -0.2, 0.2)), 0.05, 0.5),
        "counts": draw_counts(jax.random.fold_in(streams_of[4], 71), 0),
    }


cheb_low = 0.05
cheb_high = 2.0

def neighbours(field, counts):
    rows = field.shape[0]
    grid = field.reshape(rows, N_SUB, CX, CY, NZ)
    plane = lax.broadcasted_iota(jnp.int32, (1, 1, CX, 1, 1), 2)
    live = counts.astype(jnp.int32).reshape(1, N_SUB, 1, 1, 1)
    zero_plane = jnp.zeros_like(grid[:, :, :1])
    up_inside = jnp.concatenate([grid[:, :, 1:], zero_plane], axis=2)
    down_inside = jnp.concatenate([zero_plane, grid[:, :, :-1]], axis=2)
    firsts = grid[:, :, :1]
    after = jnp.concatenate([firsts[:, 1:], jnp.zeros_like(firsts[:, :1])], axis=1)
    lasts = jnp.sum(jnp.where(plane == live - 1, grid, jnp.float32(0.0)), axis=2, keepdims=True)
    before = jnp.concatenate([jnp.zeros_like(lasts[:, :1]), lasts[:, :-1]], axis=1)
    x_next = jnp.where(plane == live - 1, after, up_inside).reshape(field.shape)
    x_prev = jnp.where(plane == 0, before, down_inside).reshape(field.shape)
    zero_row = jnp.zeros_like(field[:, :, :1])
    y_next = jnp.concatenate([field[:, :, 1:], zero_row], axis=2)
    y_prev = jnp.concatenate([zero_row, field[:, :, :-1]], axis=2)
    zero_col = jnp.zeros_like(field[..., :1])
    z_next = jnp.concatenate([field[..., 1:], zero_col], axis=3)
    z_prev = jnp.concatenate([zero_col, field[..., :-1]], axis=3)
    return (x_next, x_prev, y_next, y_prev, z_next, z_prev)

def product(left, right):
    return lax.dot_general(left.reshape(left.shape[0], -1), right.reshape(right.shape[0], -1), (((1,), (1,)), ((), ())), precision=lax.Precision.HIGHEST)

def combine(coef, block):
    flat = jnp.dot(coef, block.reshape(block.shape[0], -1), precision=lax.Precision.HIGHEST)
    return flat.reshape(block.shape)

def lower_solve(factor, block):
    flat = jax.scipy.linalg.solve_triangular(factor, block.reshape(block.shape[0], -1), lower=True)
    return flat.reshape(block.shape)

def precondition(vector, operate, inv_diag):
    theta = 0.5 * (cheb_high + cheb_low)
    delta = 0.5 * (cheb_high - cheb_low)
    sigma = theta / delta
    remain = vector
    update = inv_diag * remain * (1.0 / theta)
    result = update
    rho = 1.0 / sigma
    for step in range(DEG - 1):
        remain = remain - operate(update)
        rho_next = 1.0 / (2.0 * sigma - rho)
        update = rho_next * rho * update + 2.0 * rho_next / delta * (inv_diag * remain)
        result = result + update
        rho = rho_next
    return result

def small_solve(coefs, lowers, lead):
    hess = jnp.zeros((ITERS * S, (ITERS + 1) * S), jnp.float32)
    for j in range(ITERS):
        for i in range(j + 1):
            hess = hess.at[j * S:(j + 1) * S, i * S:(i + 1) * S].set(coefs[j][i])
        hess = hess.at[j * S:(j + 1) * S, (j + 1) * S:(j + 2) * S].set(lowers[j])
    target = jnp.zeros((S, (ITERS + 1) * S), jnp.float32).at[:, :S].set(lead)
    normal = jnp.dot(hess, hess.T, precision=lax.Precision.HIGHEST)
    right = jnp.dot(hess, target.T, precision=lax.Precision.HIGHEST)
    factor = jnp.linalg.cholesky(normal)
    mix = jax.scipy.linalg.cho_solve((factor, True), right).T
    return (mix, hess, target)

def reference(rhs, perm, accum, counts):
    owner = jnp.arange(NXB, dtype=jnp.int32) // CX
    slot = jnp.arange(NXB, dtype=jnp.int32) % CX
    live_planes = (slot < counts.astype(jnp.int32)[owner]).astype(jnp.float32)
    mask = live_planes.reshape(1, NXB, 1, 1)
    field_perm = perm[None]
    near = neighbours(field_perm, counts)
    conduct = []
    diag = accum[None]
    for other in near:
        weight = 2.0 * field_perm * other / (field_perm + other)
        conduct.append(weight)
        diag = diag + weight
    inv_diag = mask / diag

    def operate(field):
        beside = neighbours(field, counts)
        total = diag * field
        for weight, other in zip(conduct, beside):
            total = total - weight * other
        return mask * total
    start = rhs * mask
    lead = jnp.linalg.cholesky(product(start, start))
    basis = [lower_solve(lead, start)]
    coefs = []
    lowers = []
    for step in range(ITERS):
        work = operate(precondition(basis[step], operate, inv_diag))
        found = [product(work, basis[i]) for i in range(step + 1)]
        for i in range(step + 1):
            work = work - combine(found[i], basis[i])
        lower = jnp.linalg.cholesky(product(work, work))
        basis.append(lower_solve(lower, work))
        coefs.append(found)
        lowers.append(lower)
    mix, hess, target = small_solve(coefs, lowers, lead)
    combo = combine(mix[:, :S], basis[0])
    for j in range(1, ITERS):
        combo = combo + combine(mix[:, j * S:(j + 1) * S], basis[j])
    solution = precondition(combo, operate, inv_diag)
    residual = start - operate(solution)
    return (solution, residual)
```

```python
import functools

import jax
import jax.numpy as jnp
from jax import lax
from jax.experimental import pallas as pl
from jax.experimental.pallas import tpu as pltpu
from jax.sharding import PartitionSpec as P

S = 8
ITERS = 4
DEG = 4


cheb_low = 0.05
cheb_high = 2.0


def with_halo(cells, sides, width):
    for axis, dim in sides:
        count = lax.axis_size(axis)
        ends = count - 1
        head = lax.slice_in_dim(cells, 0, width, axis=dim)
        tail = lax.slice_in_dim(cells, cells.shape[dim] - width, cells.shape[dim], axis=dim)
        cells = jnp.concatenate(
            [
                lax.ppermute(tail, axis, [(i, (i + 1) % count) for i in range(ends)]),
                cells,
                lax.ppermute(head, axis, [((i + 1) % count, i) for i in range(ends)]),
            ],
            axis=dim,
        )
    return cells


def neighbours(field, live, plane):
    first = field[:, 0]
    last = lax.dynamic_index_in_dim(field, live - 1, 1, keepdims=False)
    edges = with_halo(jnp.stack([first, last], axis=1), (("sub", 1),), 1)
    before = edges[:, 0:1]
    after = edges[:, 3:4]
    zero_plane = jnp.zeros_like(field[:, :1])
    up_inside = jnp.concatenate([field[:, 1:], zero_plane], axis=1)
    down_inside = jnp.concatenate([zero_plane, field[:, :-1]], axis=1)
    x_next = jnp.where(plane == live - 1, after, up_inside)
    x_prev = jnp.where(plane == 0, before, down_inside)
    zero_row = jnp.zeros_like(field[:, :, :1])
    y_next = jnp.concatenate([field[:, :, 1:], zero_row], axis=2)
    y_prev = jnp.concatenate([zero_row, field[:, :, :-1]], axis=2)
    padded = with_halo(field, (("slab", 3),), 1)
    z_next = padded[..., 2:]
    z_prev = padded[..., :-2]
    return (x_next, x_prev, y_next, y_prev, z_next, z_prev)


def product(left, right):
    return lax.dot_general(
        left.reshape(left.shape[0], -1),
        right.reshape(right.shape[0], -1),
        (((1,), (1,)), ((), ())),
        precision=lax.Precision.HIGHEST,
    )


def combine(coef, block):
    flat = jnp.dot(coef, block.reshape(block.shape[0], -1), precision=lax.Precision.HIGHEST)
    return flat.reshape(block.shape)


def lower_solve(factor, block):
    flat = jax.scipy.linalg.solve_triangular(factor, block.reshape(block.shape[0], -1), lower=True)
    return flat.reshape(block.shape)


def precondition(vector, operate, inv_diag):
    theta = 0.5 * (cheb_high + cheb_low)
    delta = 0.5 * (cheb_high - cheb_low)
    sigma = theta / delta
    remain = vector
    update = inv_diag * remain * (1.0 / theta)
    result = update
    rho = 1.0 / sigma
    for step in range(DEG - 1):
        remain = remain - operate(update)
        rho_next = 1.0 / (2.0 * sigma - rho)
        update = rho_next * rho * update + 2.0 * rho_next / delta * (inv_diag * remain)
        result = result + update
        rho = rho_next
    return result


def small_solve(coefs, lowers, lead):
    hess = jnp.zeros((ITERS * S, (ITERS + 1) * S), jnp.float32)
    for j in range(ITERS):
        for i in range(j + 1):
            hess = hess.at[j * S : (j + 1) * S, i * S : (i + 1) * S].set(coefs[j][i])
        hess = hess.at[j * S : (j + 1) * S, (j + 1) * S : (j + 2) * S].set(lowers[j])
    target = jnp.zeros((S, (ITERS + 1) * S), jnp.float32).at[:, :S].set(lead)
    normal = jnp.dot(hess, hess.T, precision=lax.Precision.HIGHEST)
    right = jnp.dot(hess, target.T, precision=lax.Precision.HIGHEST)
    factor = jnp.linalg.cholesky(normal)
    mix = jax.scipy.linalg.cho_solve((factor, True), right).T
    return (mix, hess, target)


def body(rhs, perm, accum, counts):
    live = counts[lax.axis_index("sub")]
    depth = rhs.shape[1]
    plane = lax.broadcasted_iota(jnp.int32, (1, depth, 1, 1), 1)
    mask = (plane < live).astype(jnp.float32)
    field_perm = perm[None]
    near = neighbours(field_perm, live, plane)
    conduct = []
    diag = accum[None]
    for other in near:
        weight = 2.0 * field_perm * other / (field_perm + other)
        conduct.append(weight)
        diag = diag + weight
    inv_diag = mask / diag

    def operate(field):
        beside = neighbours(field, live, plane)
        total = diag * field
        for weight, other in zip(conduct, beside):
            total = total - weight * other
        return mask * total

    start = rhs * mask
    lead = jnp.linalg.cholesky(lax.psum(product(start, start), ("sub", "slab")))
    basis = [lower_solve(lead, start)]
    coefs = []
    lowers = []
    for step in range(ITERS):
        direction = precondition(basis[step], operate, inv_diag)
        work = operate(direction)
        stacked, whole = lax.psum(
            (jnp.stack([product(work, basis[i]) for i in range(step + 1)]), product(work, work)),
            ("sub", "slab"),
        )
        found = [stacked[i] for i in range(step + 1)]
        block = whole
        for i in range(step + 1):
            work = work - combine(found[i], basis[i])
            block = block - jnp.dot(found[i], found[i].T, precision=lax.Precision.HIGHEST)
        lower = jnp.linalg.cholesky(block)
        basis.append(lower_solve(lower, work))
        coefs.append(found)
        lowers.append(lower)
    mix, hess, target = small_solve(coefs, lowers, lead)
    combo = combine(mix[:, :S], basis[0])
    for j in range(1, ITERS):
        combo = combo + combine(mix[:, j * S : (j + 1) * S], basis[j])
    solution = precondition(combo, operate, inv_diag)
    residual = start - operate(solution)
    return (solution, residual)

LANES = 128


def full(dims, left, right):
    return lax.dot_general(
        left,
        right,
        (dims, ((), ())),
        precision=lax.Precision.HIGHEST,
        preferred_element_type=jnp.float32,
    )


def chebyshev_steps():
    theta = 0.5 * (cheb_high + cheb_low)
    delta = 0.5 * (cheb_high - cheb_low)
    sigma = theta / delta
    rho = 1.0 / sigma
    steps = []
    for _ in range(DEG - 1):
        rho_next = 1.0 / (2.0 * sigma - rho)
        steps.append((rho_next * rho, 2.0 * rho_next / delta))
        rho = rho_next
    return 1.0 / theta, steps


def eliminate(mat, rows, jordan):
    row = lax.broadcasted_iota(jnp.int32, mat.shape, 0)
    for k in range(rows):
        column = jnp.broadcast_to(mat[:, k : k + 1], mat.shape)
        pivot = column[k : k + 1, :]
        line = mat[k : k + 1, :]
        if jordan:
            scaled = line / pivot
            mat = jnp.where(row == k, scaled, mat - column * scaled)
        else:
            root = lax.rsqrt(pivot)
            root = root * (1.5 - 0.5 * pivot * root * root)
            scaled = line * root
            mat = jnp.where(row == k, scaled, jnp.where(row > k, mat - column * root * scaled, mat))
    return mat


def kernel(
    dims,
    raw_ref, pick_ref, out_ref,
    ext, coef, big, near_lo, near_hi, d0, d1, rem, sol, start_own,
    part, got1, mid, got2, tmp, hess, normal,
    xs_send, xs_recv, halo_send, halo_recv, s1_send, s1_recv, s2_send, s2_recv,
):
    nsub, nslab, zl, yl_n, pack, nx = dims
    halo = DEG
    pad = halo + 1
    span = zl + 2 * halo
    per = yl_n + 1
    sub = lax.axis_index("sub")
    slab = lax.axis_index("slab")
    place = slab * nsub + sub
    total = nsub * nslab
    nxt = lax.rem(place + 1, total)
    prv = lax.rem(place + total - 1, total)

    def dev(g):
        return {"sub": lax.rem(g, nsub), "slab": g // nsub}

    barrier = pltpu.get_barrier_semaphore()
    for d in range(1, nslab):
        pl.semaphore_signal(
            barrier, inc=1, device_id={"slab": lax.rem(slab + d, nslab)}, device_id_type=pl.DeviceIdType.MESH
        )
    for d in range(1, nsub):
        pl.semaphore_signal(
            barrier, inc=1, device_id={"sub": lax.rem(sub + d, nsub)}, device_id_type=pl.DeviceIdType.MESH
        )
    for g in (nxt, prv):
        pl.semaphore_signal(barrier, inc=1, device_id=dev(g), device_id_type=pl.DeviceIdType.MESH)

    def remote(src, dst, send, recv, device):
        return pltpu.make_async_remote_copy(
            src_ref=src, dst_ref=dst, send_sem=send, recv_sem=recv,
            device_id=device, device_id_type=pl.DeviceIdType.MESH,
        )

    packed = full(((1,), (0,)), raw_ref[...], pick_ref[...])
    for k in range(zl * per):
        at = (pad * per + k) * LANES
        ext[:, at : at + LANES] = packed[k * 8 : k * 8 + 8, :]
    pl.semaphore_wait(barrier, nslab + nsub)

    edge = pad * per * LANES
    whole = zl * per * LANES
    up = remote(ext.at[:, whole : whole + edge], ext.at[:, 0:edge], xs_send.at[0], xs_recv.at[0], dev(nxt))
    down = remote(ext.at[:, edge : 2 * edge], ext.at[:, edge + whole : 2 * edge + whole], xs_send.at[1], xs_recv.at[1], dev(prv))
    up.start()
    down.start()

    lane = lax.broadcasted_iota(jnp.int32, (8, LANES), 1)
    row = lax.broadcasted_iota(jnp.int32, (8, LANES), 0)
    tile = yl_n * LANES
    own_lo, own_hi = halo * tile, (halo + zl) * tile

    for k in range(zl):
        a = (pad + k) * per * LANES
        start_own[:, k * tile : (k + 1) * tile] = ext[:, a : a + tile]
    part[...] = jnp.zeros_like(part)

    def reduce_begin(r, gram, width):
        part[r, :, 0:width] = gram
        got1[r, slab] = part[r]
        copies = []
        for d in range(1, nslab):
            peer = lax.rem(slab + d, nslab)
            c = remote(part.at[r], got1.at[r, slab], s1_send.at[r, d], s1_recv.at[r, slab], {"slab": peer})
            c.start()
            copies.append(c)
        return copies

    def reduce_end(r, copies):
        for d in range(1, nslab):
            peer = lax.rem(slab + d, nslab)
            remote(part.at[r], got1.at[r, peer], s1_send.at[r, d], s1_recv.at[r, peer], {"slab": peer}).wait_recv()
        acc = got1[r, 0]
        for i in range(1, nslab):
            acc = acc + got1[r, i]
        mid[r] = acc
        got2[r, sub] = acc
        for d in range(1, nsub):
            peer = lax.rem(sub + d, nsub)
            c = remote(mid.at[r], got2.at[r, sub], s2_send.at[r, d], s2_recv.at[r, sub], {"sub": peer})
            c.start()
            copies.append(c)
        for d in range(1, nsub):
            peer = lax.rem(sub + d, nsub)
            remote(mid.at[r], got2.at[r, peer], s2_send.at[r, d], s2_recv.at[r, peer], {"sub": peer}).wait_recv()
        acc = got2[r, 0]
        for i in range(1, nsub):
            acc = acc + got2[r, i]
        for c in copies:
            c.wait_send()
        return acc

    begun = reduce_begin(0, full(((1,), (1,)), start_own[...], start_own[...]), 8)

    up.wait()
    down.wait()
    low = jnp.where(place == 0, 0.0, 1.0).astype(jnp.float32)
    high = jnp.where(place == total - 1, 0.0, 1.0).astype(jnp.float32)
    for k in range(pad):
        a = (k * per + yl_n) * LANES
        ext[:, a : a + LANES] = ext[:, a : a + LANES] * low
        b = ((pad + zl + k) * per + yl_n) * LANES
        ext[:, b : b + LANES] = ext[:, b : b + LANES] * high
    along = lax.rem(lane, nx)

    def fill(e, _):
        def grab(t):
            return ext[:, pl.ds(pl.multiple_of(((e + 1 + t) * per + yl_n) * LANES, LANES), LANES)]

        here, after, before = grab(0), grab(1), grab(-1)
        swap_up = pltpu.roll(here, LANES - nx, 1)
        swap_down = pltpu.roll(here, nx, 1)
        x_up = jnp.where(along == nx - 1, 0.0, pltpu.roll(here, LANES - 1, 1))
        x_down = jnp.where(along == 0, 0.0, pltpu.roll(here, 1, 1))
        swap_up = jnp.where(lane >= LANES - nx, 0.0, swap_up)
        swap_down = jnp.where(lane < nx, 0.0, swap_down)

        def line(value, y):
            return jnp.broadcast_to(value[y : y + 1, :], (8, LANES))

        for y in range(yl_n):
            p = line(here, y)
            others = (
                line(x_up, y),
                line(x_down, y),
                line(here, y + 1) if y + 1 < yl_n else line(swap_up, 0),
                line(here, y - 1) if y > 0 else line(swap_down, yl_n - 1),
                line(after, y),
                line(before, y),
            )
            at = pl.ds(pl.multiple_of((e * yl_n + y) * LANES, LANES), LANES)
            diag = line(here, yl_n + y)
            for k, q in enumerate(others):
                both = p * q
                weight = jnp.where(both > 0.0, 2.0 * both / jnp.where(both > 0.0, p + q, 1.0), 0.0)
                coef[1 + k, :, at] = weight
                diag = diag + weight
            coef[0, :, at] = diag
            coef[7, :, at] = jnp.where(diag > 0.0, 1.0 / jnp.where(diag > 0.0, diag, 1.0), 0.0)
            big[0:8, at] = ext[:, pl.ds(pl.multiple_of(((e + 1) * per + y) * LANES, LANES), LANES)]
        return 0

    lax.fori_loop(0, span, fill, 0)

    first, steps = chebyshev_steps()

    def spot(e, y):
        return pl.ds(pl.multiple_of((e * yl_n + y) * LANES, LANES), LANES)

    def stencil(field, e):
        here = [field[:, spot(e, y)] for y in range(yl_n)]
        outs = []
        for y in range(yl_n):
            at = spot(e, y)
            f = here[y]
            y_up = here[y + 1] if y + 1 < yl_n else pltpu.roll(here[0], LANES - nx, 1)
            y_down = here[y - 1] if y > 0 else pltpu.roll(here[yl_n - 1], nx, 1)
            acc = coef[0, :, at] * f
            acc = acc - coef[1, :, at] * pltpu.roll(f, LANES - 1, 1)
            acc = acc - coef[2, :, at] * pltpu.roll(f, 1, 1)
            acc = acc - coef[3, :, at] * y_up
            acc = acc - coef[4, :, at] * y_down
            acc = acc - coef[5, :, at] * field[:, spot(e + 1, y)]
            acc = acc - coef[6, :, at] * field[:, spot(e - 1, y)]
            outs.append(acc)
        return here, outs

    def precondition_ref(load):
        def begin(e, _):
            for y in range(yl_n):
                at = spot(e, y)
                v = load(at)
                d = coef[7, :, at] * v * first
                rem[:, at] = v
                d0[:, at] = d
                sol[:, at] = d
            return 0

        lax.fori_loop(0, span, begin, 0)
        source, target = d0, d1
        for t, (keep, gain) in enumerate(steps):
            def one(e, _, source=source, target=target, keep=keep, gain=gain):
                here, outs = stencil(source, e)
                for y in range(yl_n):
                    at = spot(e, y)
                    r = rem[:, at] - outs[y]
                    rem[:, at] = r
                    d = keep * here[y] + gain * (coef[7, :, at] * r)
                    target[:, at] = d
                    sol[:, at] = sol[:, at] + d
                return 0

            lax.fori_loop(t + 1, span - t - 1, one, 0)
            source, target = target, source

    summed = reduce_end(0, begun)
    lead_mat = jnp.where(lane < 8, summed, 0.0) + jnp.where(lane == row + 64, 1.0, 0.0)
    done = eliminate(lead_mat, 8, False)
    lead_t = jnp.where(lane < 8, done, 0.0)
    inverse = pltpu.roll(done, 64, 1)
    big[8:16, :] = full(((1,), (0,)), inverse[:, 0:8], big[0:8, :])

    side = halo * tile
    for j in range(ITERS):
        r = j + 1
        base = 8 * (j + 1)
        precondition_ref(lambda at, base=base: big[base : base + 8, at])

        def apply(e, _):
            _, outs = stencil(sol, e)
            for y in range(yl_n):
                big[0:8, spot(e, y)] = outs[y]
            return 0

        lax.fori_loop(halo, halo + zl, apply, 0)
        moves = []
        if j < ITERS - 1:
            moves = [
                remote(big.at[0:8, own_hi - side : own_hi], near_lo.at[j], halo_send.at[j, 0], halo_recv.at[j, 0], dev(nxt)),
                remote(big.at[0:8, own_lo : own_lo + side], near_hi.at[j], halo_send.at[j, 1], halo_recv.at[j, 1], dev(prv)),
            ]
        width = 8 * (j + 2)
        gram = full(((1,), (1,)), big[0:8, own_lo:own_hi], big[0:width, own_lo:own_hi])
        begun = reduce_begin(r, gram, width)
        for m in moves:
            m.start()
        summed = reduce_end(r, begun)
        only = jnp.where(lane >= 8, summed, 0.0)
        tmp[...] = only + jnp.where(lane == row + 64, 1.0, 0.0)
        tmp[:, 0:8] = summed[:, 0:8] - full(((1,), (1,)), only, only)
        done = eliminate(tmp[...], 8, False)
        hess[8 * j : 8 * j + 8, :] = jnp.where(lane < base, pltpu.roll(summed, LANES - 8, 1), 0.0)
        hess[8 * j : 8 * j + 8, base : base + 8] = done.T[0:8, :]
        if j < ITERS - 1:
            for m in moves:
                m.wait()
            big[0:8, 0:own_lo] = near_lo[j]
            big[0:8, own_hi : own_hi + side] = near_hi[j]
            mixer = jnp.where(lane < 8, pltpu.roll(done, 64, 1), -done)
            big[base + 8 : base + 16, :] = full(((1,), (0,)), mixer[:, 0:width], big[0:width, :])

    rows = 8 * ITERS
    h = hess[...]
    normal[...] = jnp.zeros_like(normal)
    normal[:, 0:rows] = full(((1,), (1,)), h, h)
    normal[:, rows : rows + 8] = full(((1,), (0,)), h[:, 0:8], lead_t[:, 0:8])
    solved = eliminate(normal[...], rows, True)
    mix = solved.T[rows : rows + 8, :]
    big[0:8, :] = full(((1,), (0,)), mix, big[8 : 8 + rows, :])
    precondition_ref(lambda at: big[0:8, at])

    def finish(e, _):
        _, outs = stencil(sol, e)
        for y in range(yl_n):
            k = pl.multiple_of(((e - halo) * yl_n + y) * LANES, LANES)
            w = pl.multiple_of(((e - halo) * yl_n + y) * 8, 8)
            d0_at = pl.ds(w, 8)
            out_ref[0, d0_at, :] = sol[:, spot(e, y)]
            out_ref[1, d0_at, :] = start_own[:, pl.ds(k, LANES)] - outs[y]
        return 0

    lax.fori_loop(halo, halo + zl, finish, 0)
    for f in range(2):
        out_ref[f] = full(((1,), (1,)), out_ref[f], pick_ref[...])


def fast_body(rhs, perm, accum, counts):
    nsub, nslab = lax.axis_size("sub"), lax.axis_size("slab")
    s, depth, cy, zs = rhs.shape
    nx = depth * nsub
    pack = LANES // nx
    yl = cy // pack
    zl = zs // nsub
    span = zl + 2 * DEG
    pad = DEG + 1

    def turn(a):
        k = a.shape[0]
        a = a.reshape(k, depth, pack, yl, nsub, zl)
        return jnp.transpose(a, (4, 5, 3, 0, 2, 1)).reshape(nsub, zl, yl, k, pack * depth)

    fields = turn(rhs)
    pa = jnp.transpose(turn(jnp.stack([perm, accum])), (0, 1, 3, 2, 4)).reshape(nsub, zl, 1, 2 * yl, pack * depth)
    send = jnp.concatenate([fields, pa], axis=2)
    got = lax.all_to_all(send, "sub", 0, 0)
    raw = jnp.transpose(got, (1, 2, 3, 0, 4)).reshape(zl * (yl + 1) * s, LANES)

    before = jnp.cumsum(counts) - counts
    slot = jnp.arange(depth, dtype=jnp.int32)
    goal = jnp.where(slot[None] < counts[:, None], before[:, None] + slot[None], -1)
    half = jnp.arange(pack, dtype=jnp.int32)[None, :, None]
    goal = jnp.where(goal[:, None, :] >= 0, goal[:, None, :] + half * nx, -1).reshape(LANES, 1)
    pick = (goal == jnp.arange(LANES, dtype=jnp.int32)[None]).astype(jnp.float32)

    wide = span * yl * LANES
    f32 = jnp.float32
    rounds = ITERS + 1
    side = DEG * yl * LANES
    dma = pltpu.SemaphoreType.DMA
    out = pl.pallas_call(
        functools.partial(kernel, (nsub, nslab, zl, yl, pack, nx)),
        out_shape=jax.ShapeDtypeStruct((2, zl * yl * s, LANES), f32),
        in_specs=[pl.BlockSpec(memory_space=pltpu.VMEM)] * 2,
        out_specs=pl.BlockSpec(memory_space=pltpu.VMEM),
        scratch_shapes=[
            pltpu.VMEM((8, (zl + 2 * pad) * (yl + 1) * LANES), f32),
            pltpu.VMEM((8, 8, wide), f32),
            pltpu.VMEM((8 * (ITERS + 1), wide), f32),
            pltpu.VMEM((ITERS - 1, 8, side), f32),
            pltpu.VMEM((ITERS - 1, 8, side), f32),
            pltpu.VMEM((8, wide), f32),
            pltpu.VMEM((8, wide), f32),
            pltpu.VMEM((8, wide), f32),
            pltpu.VMEM((8, wide), f32),
            pltpu.VMEM((8, zl * yl * LANES), f32),
            pltpu.VMEM((rounds, 8, LANES), f32),
            pltpu.VMEM((rounds, nslab, 8, LANES), f32),
            pltpu.VMEM((rounds, 8, LANES), f32),
            pltpu.VMEM((rounds, nsub, 8, LANES), f32),
            pltpu.VMEM((8, LANES), f32),
            pltpu.VMEM((8 * ITERS, LANES), f32),
            pltpu.VMEM((8 * ITERS, LANES), f32),
            dma((2,)),
            dma((2,)),
            dma((ITERS - 1, 2)),
            dma((ITERS - 1, 2)),
            dma((rounds, nslab)),
            dma((rounds, nslab)),
            dma((rounds, nsub)),
            dma((rounds, nsub)),
        ],
        compiler_params=pltpu.CompilerParams(
            collective_id=0, has_side_effects=True, vmem_limit_bytes=48 * 1024 * 1024
        ),
    )(raw, pick)
    back = out.reshape(2, zl, yl, s, nsub, pack * depth)
    back = jnp.transpose(back, (4, 0, 1, 2, 3, 5))
    back = lax.all_to_all(back, "sub", 0, 0)
    back = back.reshape(nsub, 2, zl, yl, s, pack, depth)
    back = jnp.transpose(back, (1, 4, 6, 5, 3, 0, 2)).reshape(2, s, depth, cy, zs)
    return back[0], back[1]


def choose(rhs, perm, accum, counts):
    nsub = lax.axis_size("sub")
    s, depth, cy, zs = rhs.shape
    nx = depth * nsub
    fits = s == S == 8 and LANES % nx == 0 and zs % nsub == 0 and zs // nsub > DEG
    fits = fits and cy % max(LANES // nx, 1) == 0 and cy // max(LANES // nx, 1) == 4
    if fits:
        return fast_body(rhs, perm, accum, counts)
    return body(rhs, perm, accum, counts)


def solution(mesh):
    placed = (P(None, "sub", None, "slab"), P("sub", None, "slab"), P("sub", None, "slab"), P())
    return jax.shard_map(
        choose,
        mesh=mesh,
        in_specs=placed,
        out_specs=(P(None, "sub", None, "slab"), P(None, "sub", None, "slab")),
        check_vma=False,
    )
```

```python
import functools

import jax
import jax.numpy as jnp
from jax import lax
from jax.experimental import pallas as pl
from jax.experimental.pallas import tpu as pltpu
from jax.sharding import PartitionSpec as P

S = 8
ITERS = 4
DEG = 4


cheb_low = 0.05
cheb_high = 2.0


def with_halo(cells, sides, width):
    for axis, dim in sides:
        count = lax.axis_size(axis)
        ends = count - 1
        head = lax.slice_in_dim(cells, 0, width, axis=dim)
        tail = lax.slice_in_dim(cells, cells.shape[dim] - width, cells.shape[dim], axis=dim)
        cells = jnp.concatenate(
            [
                lax.ppermute(tail, axis, [(i, (i + 1) % count) for i in range(ends)]),
                cells,
                lax.ppermute(head, axis, [((i + 1) % count, i) for i in range(ends)]),
            ],
            axis=dim,
        )
    return cells


def neighbours(field, live, plane):
    first = field[:, 0]
    last = lax.dynamic_index_in_dim(field, live - 1, 1, keepdims=False)
    edges = with_halo(jnp.stack([first, last], axis=1), (("sub", 1),), 1)
    before = edges[:, 0:1]
    after = edges[:, 3:4]
    zero_plane = jnp.zeros_like(field[:, :1])
    up_inside = jnp.concatenate([field[:, 1:], zero_plane], axis=1)
    down_inside = jnp.concatenate([zero_plane, field[:, :-1]], axis=1)
    x_next = jnp.where(plane == live - 1, after, up_inside)
    x_prev = jnp.where(plane == 0, before, down_inside)
    zero_row = jnp.zeros_like(field[:, :, :1])
    y_next = jnp.concatenate([field[:, :, 1:], zero_row], axis=2)
    y_prev = jnp.concatenate([zero_row, field[:, :, :-1]], axis=2)
    padded = with_halo(field, (("slab", 3),), 1)
    z_next = padded[..., 2:]
    z_prev = padded[..., :-2]
    return (x_next, x_prev, y_next, y_prev, z_next, z_prev)


def product(left, right):
    return lax.dot_general(
        left.reshape(left.shape[0], -1),
        right.reshape(right.shape[0], -1),
        (((1,), (1,)), ((), ())),
        precision=lax.Precision.HIGHEST,
    )


def combine(coef, block):
    flat = jnp.dot(coef, block.reshape(block.shape[0], -1), precision=lax.Precision.HIGHEST)
    return flat.reshape(block.shape)


def lower_solve(factor, block):
    flat = jax.scipy.linalg.solve_triangular(factor, block.reshape(block.shape[0], -1), lower=True)
    return flat.reshape(block.shape)


def precondition(vector, operate, inv_diag):
    theta = 0.5 * (cheb_high + cheb_low)
    delta = 0.5 * (cheb_high - cheb_low)
    sigma = theta / delta
    remain = vector
    update = inv_diag * remain * (1.0 / theta)
    result = update
    rho = 1.0 / sigma
    for step in range(DEG - 1):
        remain = remain - operate(update)
        rho_next = 1.0 / (2.0 * sigma - rho)
        update = rho_next * rho * update + 2.0 * rho_next / delta * (inv_diag * remain)
        result = result + update
        rho = rho_next
    return result


def small_solve(coefs, lowers, lead):
    hess = jnp.zeros((ITERS * S, (ITERS + 1) * S), jnp.float32)
    for j in range(ITERS):
        for i in range(j + 1):
            hess = hess.at[j * S : (j + 1) * S, i * S : (i + 1) * S].set(coefs[j][i])
        hess = hess.at[j * S : (j + 1) * S, (j + 1) * S : (j + 2) * S].set(lowers[j])
    target = jnp.zeros((S, (ITERS + 1) * S), jnp.float32).at[:, :S].set(lead)
    normal = jnp.dot(hess, hess.T, precision=lax.Precision.HIGHEST)
    right = jnp.dot(hess, target.T, precision=lax.Precision.HIGHEST)
    factor = jnp.linalg.cholesky(normal)
    mix = jax.scipy.linalg.cho_solve((factor, True), right).T
    return (mix, hess, target)


def body(rhs, perm, accum, counts):
    live = counts[lax.axis_index("sub")]
    depth = rhs.shape[1]
    plane = lax.broadcasted_iota(jnp.int32, (1, depth, 1, 1), 1)
    mask = (plane < live).astype(jnp.float32)
    field_perm = perm[None]
    near = neighbours(field_perm, live, plane)
    conduct = []
    diag = accum[None]
    for other in near:
        weight = 2.0 * field_perm * other / (field_perm + other)
        conduct.append(weight)
        diag = diag + weight
    inv_diag = mask / diag

    def operate(field):
        beside = neighbours(field, live, plane)
        total = diag * field
        for weight, other in zip(conduct, beside):
            total = total - weight * other
        return mask * total

    start = rhs * mask
    lead = jnp.linalg.cholesky(lax.psum(product(start, start), ("sub", "slab")))
    basis = [lower_solve(lead, start)]
    coefs = []
    lowers = []
    for step in range(ITERS):
        direction = precondition(basis[step], operate, inv_diag)
        work = operate(direction)
        stacked, whole = lax.psum(
            (jnp.stack([product(work, basis[i]) for i in range(step + 1)]), product(work, work)),
            ("sub", "slab"),
        )
        found = [stacked[i] for i in range(step + 1)]
        block = whole
        for i in range(step + 1):
            work = work - combine(found[i], basis[i])
            block = block - jnp.dot(found[i], found[i].T, precision=lax.Precision.HIGHEST)
        lower = jnp.linalg.cholesky(block)
        basis.append(lower_solve(lower, work))
        coefs.append(found)
        lowers.append(lower)
    mix, hess, target = small_solve(coefs, lowers, lead)
    combo = combine(mix[:, :S], basis[0])
    for j in range(1, ITERS):
        combo = combo + combine(mix[:, j * S : (j + 1) * S], basis[j])
    solution = precondition(combo, operate, inv_diag)
    residual = start - operate(solution)
    return (solution, residual)

LANES = 128


def full(dims, left, right):
    return lax.dot_general(
        left,
        right,
        (dims, ((), ())),
        precision=lax.Precision.HIGHEST,
        preferred_element_type=jnp.float32,
    )


def chebyshev_steps():
    theta = 0.5 * (cheb_high + cheb_low)
    delta = 0.5 * (cheb_high - cheb_low)
    sigma = theta / delta
    rho = 1.0 / sigma
    steps = []
    for _ in range(DEG - 1):
        rho_next = 1.0 / (2.0 * sigma - rho)
        steps.append((rho_next * rho, 2.0 * rho_next / delta))
        rho = rho_next
    return 1.0 / theta, steps


def eliminate(mat, rows, jordan):
    row = lax.broadcasted_iota(jnp.int32, mat.shape, 0)
    for k in range(rows):
        column = jnp.broadcast_to(mat[:, k : k + 1], mat.shape)
        pivot = column[k : k + 1, :]
        line = mat[k : k + 1, :]
        if jordan:
            scaled = line / pivot
            mat = jnp.where(row == k, scaled, mat - column * scaled)
        else:
            root = lax.rsqrt(pivot)
            root = root * (1.5 - 0.5 * pivot * root * root)
            scaled = line * root
            mat = jnp.where(row == k, scaled, jnp.where(row > k, mat - column * root * scaled, mat))
    return mat


def kernel(
    dims,
    rhs_ref, perm_ref, accum_ref, counts_ref, out0_ref, out1_ref,
    pick_ref, raw_ref, out_ref, in_buf, in_got, out_buf, out_got,
    ext, coef, big, near_lo, near_hi, d0, d1, rem, sol, start_own,
    part, got1, mid, got2, tmp, hess, normal,
    in_send, in_recv, out_send, out_recv, xs_send, xs_recv, halo_send, halo_recv, s1_send, s1_recv, s2_send, s2_recv,
):
    nsub, nslab, zl, yl_n, pack, nx = dims
    halo = DEG
    pad = halo + 1
    span = zl + 2 * halo
    per = yl_n + 1
    sub = lax.axis_index("sub")
    slab = lax.axis_index("slab")
    place = slab * nsub + sub
    total = nsub * nslab
    nxt = lax.rem(place + 1, total)
    prv = lax.rem(place + total - 1, total)

    def dev(g):
        return {"sub": lax.rem(g, nsub), "slab": g // nsub}

    barrier = pltpu.get_barrier_semaphore()
    for d in range(1, nslab):
        pl.semaphore_signal(
            barrier, inc=1, device_id={"slab": lax.rem(slab + d, nslab)}, device_id_type=pl.DeviceIdType.MESH
        )
    for d in range(1, nsub):
        pl.semaphore_signal(
            barrier, inc=1, device_id={"sub": lax.rem(sub + d, nsub)}, device_id_type=pl.DeviceIdType.MESH
        )
    for g in (nxt, prv):
        pl.semaphore_signal(barrier, inc=1, device_id=dev(g), device_id_type=pl.DeviceIdType.MESH)

    def remote(src, dst, send, recv, device):
        return pltpu.make_async_remote_copy(
            src_ref=src, dst_ref=dst, send_sem=send, recv_sem=recv,
            device_id=device, device_id_type=pl.DeviceIdType.MESH,
        )

    group = pack * (LANES // (pack * nsub))
    wide_row = lax.broadcasted_iota(jnp.int32, (LANES, LANES), 0)
    wide_lane = lax.broadcasted_iota(jnp.int32, (LANES, LANES), 1)
    rank = lax.rem(wide_row, group) // pack
    owner = wide_row // group
    base_of = jnp.zeros_like(wide_row)
    live_of = jnp.zeros_like(wide_row)
    before = jnp.int32(0)
    for i in range(nsub):
        live = counts_ref[i]
        base_of = jnp.where(owner == i, before, base_of)
        live_of = jnp.where(owner == i, live, live_of)
        before = before + live
    goal = base_of + rank + lax.rem(wide_row, pack) * nx
    pick_ref[...] = jnp.where((rank < live_of) & (goal == wide_lane), 1.0, 0.0).astype(jnp.float32)

    for y in range(yl_n):
        in_buf[y] = rhs_ref[pl.ds(y, LANES, stride=yl_n), :].T
    pieces = [ref[pl.ds(y, group, stride=yl_n), :] for ref in (perm_ref, accum_ref) for y in range(yl_n)]
    in_buf[yl_n] = jnp.concatenate(pieces, axis=0).T

    pl.semaphore_wait(barrier, nslab + nsub)

    def rows_of(i):
        return pl.ds(pl.multiple_of(i * zl, 8), zl)

    arrivals = []
    for d in range(1, nsub):
        peer = lax.rem(sub + d, nsub)
        c = remote(in_buf.at[:, rows_of(peer), :], in_got.at[sub], in_send.at[d], in_recv.at[sub], {"sub": peer})
        c.start()
        arrivals.append(c)
    in_got[sub] = in_buf[:, rows_of(sub), :]
    for d in range(1, nsub):
        peer = lax.rem(sub + d, nsub)
        remote(in_buf.at[:, rows_of(peer), :], in_got.at[peer], in_send.at[d], in_recv.at[peer], {"sub": peer}).wait_recv()

    strip = lax.broadcasted_iota(jnp.int32, (zl, LANES), 1) // group

    def butterfly(items):
        d = len(items) // 2
        while d:
            fresh = list(items)
            for a in range(len(items)):
                if a & d:
                    continue
                first_half = (strip & d) == 0
                fresh[a] = jnp.where(first_half, items[a], pltpu.roll(items[a + d], group * d, 1))
                fresh[a + d] = jnp.where(first_half, pltpu.roll(items[a], LANES - group * d, 1), items[a + d])
            items = fresh
            d //= 2
        return items

    for t in range(per):
        for i, value in enumerate(butterfly([in_got[i, t] for i in range(nsub)])):
            raw_ref[pl.ds(t * 8 + i, zl, stride=per * 8), :] = value

    packed = full(((1,), (0,)), raw_ref[...], pick_ref[...])
    for k in range(zl * per):
        at = (pad * per + k) * LANES
        ext[:, at : at + LANES] = packed[k * 8 : k * 8 + 8, :]
    edge = pad * per * LANES
    whole = zl * per * LANES
    up = remote(ext.at[:, whole : whole + edge], ext.at[:, 0:edge], xs_send.at[0], xs_recv.at[0], dev(nxt))
    down = remote(ext.at[:, edge : 2 * edge], ext.at[:, edge + whole : 2 * edge + whole], xs_send.at[1], xs_recv.at[1], dev(prv))
    up.start()
    down.start()

    lane = lax.broadcasted_iota(jnp.int32, (8, LANES), 1)
    row = lax.broadcasted_iota(jnp.int32, (8, LANES), 0)
    tile = yl_n * LANES
    own_lo, own_hi = halo * tile, (halo + zl) * tile

    for k in range(zl):
        a = (pad + k) * per * LANES
        start_own[:, k * tile : (k + 1) * tile] = ext[:, a : a + tile]
        big[0:8, (halo + k) * tile : (halo + k + 1) * tile] = ext[:, a : a + tile]

    def products(blocks):
        def add(k, accs):
            accs = list(accs)
            for h in range(2):
                at = pl.ds(pl.multiple_of((2 * k + h) * LANES + own_lo, LANES), LANES)
                w = big[0:8, at]
                turned = [w] + [pltpu.roll(w, n, 0) for n in range(1, 8)]
                for b in range(blocks):
                    v = w if b == 0 else big[8 * b : 8 * b + 8, at]
                    for n in range(8):
                        accs[8 * b + n] = accs[8 * b + n] + v * turned[n]
            return tuple(accs)

        zero = jnp.zeros((8, LANES), jnp.float32)
        accs = lax.fori_loop(0, zl * yl_n // 2, add, (zero,) * (8 * blocks))
        out = zero
        for b in range(blocks):
            for n in range(8):
                acc = accs[8 * b + n]
                acc = pltpu.roll(acc, 8 - n, 0) if n else acc
                line = jnp.sum(acc, axis=1, keepdims=True)
                out = jnp.where(lane == 8 * b + lax.rem(row + n, 8), line, out)
        return out

    def reduce_begin(r, gram):
        part[r] = gram
        got1[r, slab] = part[r]
        copies = []
        for d in range(1, nslab):
            peer = lax.rem(slab + d, nslab)
            c = remote(part.at[r], got1.at[r, slab], s1_send.at[r, d], s1_recv.at[r, slab], {"slab": peer})
            c.start()
            copies.append(c)
        return copies

    def reduce_end(r, copies):
        for d in range(1, nslab):
            peer = lax.rem(slab + d, nslab)
            remote(part.at[r], got1.at[r, peer], s1_send.at[r, d], s1_recv.at[r, peer], {"slab": peer}).wait_recv()
        acc = got1[r, 0]
        for i in range(1, nslab):
            acc = acc + got1[r, i]
        mid[r] = acc
        got2[r, sub] = acc
        for d in range(1, nsub):
            peer = lax.rem(sub + d, nsub)
            c = remote(mid.at[r], got2.at[r, sub], s2_send.at[r, d], s2_recv.at[r, sub], {"sub": peer})
            c.start()
            copies.append(c)
        for d in range(1, nsub):
            peer = lax.rem(sub + d, nsub)
            remote(mid.at[r], got2.at[r, peer], s2_send.at[r, d], s2_recv.at[r, peer], {"sub": peer}).wait_recv()
        acc = got2[r, 0]
        for i in range(1, nsub):
            acc = acc + got2[r, i]
        for c in copies:
            c.wait_send()
        return acc

    begun = reduce_begin(0, products(1))

    up.wait()
    down.wait()
    low = jnp.where(place == 0, 0.0, 1.0).astype(jnp.float32)
    high = jnp.where(place == total - 1, 0.0, 1.0).astype(jnp.float32)
    for k in range(pad):
        a = (k * per + yl_n) * LANES
        ext[:, a : a + LANES] = ext[:, a : a + LANES] * low
        b = ((pad + zl + k) * per + yl_n) * LANES
        ext[:, b : b + LANES] = ext[:, b : b + LANES] * high
    along = lax.rem(lane, nx)

    def fill(e, _):
        def grab(t):
            return ext[:, pl.ds(pl.multiple_of(((e + 1 + t) * per + yl_n) * LANES, LANES), LANES)]

        here, after, before = grab(0), grab(1), grab(-1)
        swap_up = pltpu.roll(here, LANES - nx, 1)
        swap_down = pltpu.roll(here, nx, 1)
        x_up = jnp.where(along == nx - 1, 0.0, pltpu.roll(here, LANES - 1, 1))
        x_down = jnp.where(along == 0, 0.0, pltpu.roll(here, 1, 1))
        swap_up = jnp.where(lane >= LANES - nx, 0.0, swap_up)
        swap_down = jnp.where(lane < nx, 0.0, swap_down)

        def line(value, y):
            return jnp.broadcast_to(value[y : y + 1, :], (8, LANES))

        for y in range(yl_n):
            p = line(here, y)
            others = (
                line(x_up, y),
                line(x_down, y),
                line(here, y + 1) if y + 1 < yl_n else line(swap_up, 0),
                line(here, y - 1) if y > 0 else line(swap_down, yl_n - 1),
                line(after, y),
                line(before, y),
            )
            at = pl.ds(pl.multiple_of((e * yl_n + y) * LANES, LANES), LANES)
            diag = line(here, yl_n + y)
            for k, q in enumerate(others):
                both = p * q
                weight = jnp.where(both > 0.0, 2.0 * both / jnp.where(both > 0.0, p + q, 1.0), 0.0)
                coef[1 + k, :, at] = weight
                diag = diag + weight
            coef[0, :, at] = diag
            coef[7, :, at] = jnp.where(diag > 0.0, 1.0 / jnp.where(diag > 0.0, diag, 1.0), 0.0)
            big[0:8, at] = ext[:, pl.ds(pl.multiple_of(((e + 1) * per + y) * LANES, LANES), LANES)]
        return 0

    lax.fori_loop(0, span, fill, 0)

    first, steps = chebyshev_steps()

    def spot(e, y):
        if isinstance(e, int):
            return pl.ds((e * yl_n + y) * LANES, LANES)
        return pl.ds(pl.multiple_of((e * yl_n + y) * LANES, LANES), LANES)

    def stencil(field, e):
        here = [field[:, spot(e, y)] for y in range(yl_n)]
        outs = []
        for y in range(yl_n):
            at = spot(e, y)
            f = here[y]
            y_up = here[y + 1] if y + 1 < yl_n else pltpu.roll(here[0], LANES - nx, 1)
            y_down = here[y - 1] if y > 0 else pltpu.roll(here[yl_n - 1], nx, 1)
            acc = coef[0, :, at] * f
            acc = acc - coef[1, :, at] * pltpu.roll(f, LANES - 1, 1)
            acc = acc - coef[2, :, at] * pltpu.roll(f, 1, 1)
            acc = acc - coef[3, :, at] * y_up
            acc = acc - coef[4, :, at] * y_down
            acc = acc - coef[5, :, at] * field[:, spot(e + 1, y)]
            acc = acc - coef[6, :, at] * field[:, spot(e - 1, y)]
            outs.append(acc)
        return here, outs

    def sweep(lo, hi, work, chunk=4):
        turns = (hi - lo) // chunk

        def one(k, _):
            work([lo + k * chunk + n for n in range(chunk)])
            return 0

        lax.fori_loop(0, turns, one, 0)
        if lo + turns * chunk < hi:
            work(list(range(lo + turns * chunk, hi)))

    def precondition_ref(load):
        def begin(es):
            for e in es:
                for y in range(yl_n):
                    at = spot(e, y)
                    v = load(at)
                    d = coef[7, :, at] * v * first
                    rem[:, at] = v
                    d0[:, at] = d
                    sol[:, at] = d

        sweep(0, span, begin)
        source, target = d0, d1
        for t, (keep, gain) in enumerate(steps):
            def one(es, source=source, target=target, keep=keep, gain=gain):
                found = [stencil(source, e) for e in es]
                for e, (here, outs) in zip(es, found):
                    for y in range(yl_n):
                        at = spot(e, y)
                        r = rem[:, at] - outs[y]
                        rem[:, at] = r
                        d = keep * here[y] + gain * (coef[7, :, at] * r)
                        target[:, at] = d
                        sol[:, at] = sol[:, at] + d

            sweep(t + 1, span - t - 1, one)
            source, target = target, source

    summed = reduce_end(0, begun)
    lead_mat = jnp.where(lane < 8, summed, 0.0) + jnp.where(lane == row + 64, 1.0, 0.0)
    done = eliminate(lead_mat, 8, False)
    lead_t = jnp.where(lane < 8, done, 0.0)
    inverse = pltpu.roll(done, 64, 1)
    big[8:16, :] = full(((1,), (0,)), inverse[:, 0:8], big[0:8, :])

    side = halo * tile
    for j in range(ITERS):
        r = j + 1
        base = 8 * (j + 1)
        precondition_ref(lambda at, base=base: big[base : base + 8, at])

        def apply(es):
            for e in es:
                _, outs = stencil(sol, e)
                for y in range(yl_n):
                    big[0:8, spot(e, y)] = outs[y]

        sweep(halo, halo + zl, apply)
        moves = []
        if j < ITERS - 1:
            moves = [
                remote(big.at[0:8, own_hi - side : own_hi], near_lo.at[j], halo_send.at[j, 0], halo_recv.at[j, 0], dev(nxt)),
                remote(big.at[0:8, own_lo : own_lo + side], near_hi.at[j], halo_send.at[j, 1], halo_recv.at[j, 1], dev(prv)),
            ]
        width = 8 * (j + 2)
        for m in moves:
            m.start()
        begun = reduce_begin(r, products(j + 2))
        summed = reduce_end(r, begun)
        only = jnp.where(lane >= 8, summed, 0.0)
        tmp[...] = only + jnp.where(lane == row + 64, 1.0, 0.0)
        tmp[:, 0:8] = summed[:, 0:8] - full(((1,), (1,)), only, only)
        done = eliminate(tmp[...], 8, False)
        hess[8 * j : 8 * j + 8, :] = jnp.where(lane < base, pltpu.roll(summed, LANES - 8, 1), 0.0)
        hess[8 * j : 8 * j + 8, base : base + 8] = done.T[0:8, :]
        if j < ITERS - 1:
            for m in moves:
                m.wait()
            big[0:8, 0:own_lo] = near_lo[j]
            big[0:8, own_hi : own_hi + side] = near_hi[j]
            mixer = jnp.where(lane < 8, pltpu.roll(done, 64, 1), -done)
            big[base + 8 : base + 16, :] = full(((1,), (0,)), mixer[:, 0:width], big[0:width, :])

    rows = 8 * ITERS
    h = hess[...]
    normal[...] = jnp.zeros_like(normal)
    normal[:, 0:rows] = full(((1,), (1,)), h, h)
    normal[:, rows : rows + 8] = full(((1,), (0,)), h[:, 0:8], lead_t[:, 0:8])
    solved = eliminate(normal[...], rows, True)
    mix = solved.T[rows : rows + 8, :]
    big[0:8, :] = full(((1,), (0,)), mix, big[8 : 8 + rows, :])
    precondition_ref(lambda at: big[0:8, at])

    def finish(es):
        for e in es:
            _, outs = stencil(sol, e)
            for y in range(yl_n):
                k = pl.multiple_of(((e - halo) * yl_n + y) * LANES, LANES)
                w = pl.multiple_of(((e - halo) * yl_n + y) * 8, 8)
                out_ref[0, pl.ds(w, 8), :] = sol[:, spot(e, y)]
                out_ref[1, pl.ds(w, 8), :] = start_own[:, pl.ds(k, LANES)] - outs[y]

    sweep(halo, halo + zl, finish)
    for f in range(2):
        raw_ref[0 : zl * yl_n * 8, :] = full(((1,), (1,)), out_ref[f], pick_ref[...])
        for y in range(yl_n):
            items = [raw_ref[pl.ds(y * 8 + i, zl, stride=yl_n * 8), :] for i in range(nsub)]
            for i, value in enumerate(butterfly(items)):
                out_buf[i, f * yl_n + y] = value
    leaving = []
    for d in range(1, nsub):
        peer = lax.rem(sub + d, nsub)
        c = remote(out_buf.at[peer], out_got.at[:, rows_of(sub), :], out_send.at[d], out_recv.at[sub], {"sub": peer})
        c.start()
        leaving.append(c)
    out_got[:, rows_of(sub), :] = out_buf[sub]
    for d in range(1, nsub):
        peer = lax.rem(sub + d, nsub)
        remote(out_buf.at[peer], out_got.at[:, rows_of(peer), :], out_send.at[d], out_recv.at[peer], {"sub": peer}).wait_recv()
    for f, ref in enumerate((out0_ref, out1_ref)):
        for y in range(yl_n):
            ref[pl.ds(y, LANES, stride=yl_n), :] = out_got[f * yl_n + y].T
    for c in arrivals + leaving:
        c.wait_send()


def fast_body(rhs, perm, accum, counts):
    nsub, nslab = lax.axis_size("sub"), lax.axis_size("slab")
    s, depth, cy, zs = rhs.shape
    nx = depth * nsub
    pack = LANES // nx
    yl = cy // pack
    zl = zs // nsub
    span = zl + 2 * DEG
    pad = DEG + 1

    wide = span * yl * LANES
    f32 = jnp.float32
    rounds = ITERS + 1
    side = DEG * yl * LANES
    dma = pltpu.SemaphoreType.DMA
    out = pl.pallas_call(
        functools.partial(kernel, (nsub, nslab, zl, yl, pack, nx)),
        out_shape=[jax.ShapeDtypeStruct((s * depth * cy, zs), f32)] * 2,
        in_specs=[pl.BlockSpec(memory_space=pltpu.VMEM)] * 3 + [pl.BlockSpec(memory_space=pltpu.SMEM)],
        out_specs=[pl.BlockSpec(memory_space=pltpu.VMEM)] * 2,
        scratch_shapes=[
            pltpu.VMEM((LANES, LANES), f32),
            pltpu.VMEM((zl * (yl + 1) * s, LANES), f32),
            pltpu.VMEM((2, zl * yl * s, LANES), f32),
            pltpu.VMEM((yl + 1, zs, LANES), f32),
            pltpu.VMEM((nsub, yl + 1, zl, LANES), f32),
            pltpu.VMEM((nsub, 2 * yl, zl, LANES), f32),
            pltpu.VMEM((2 * yl, zs, LANES), f32),
            pltpu.VMEM((8, (zl + 2 * pad) * (yl + 1) * LANES), f32),
            pltpu.VMEM((8, 8, wide), f32),
            pltpu.VMEM((8 * (ITERS + 1), wide), f32),
            pltpu.VMEM((ITERS - 1, 8, side), f32),
            pltpu.VMEM((ITERS - 1, 8, side), f32),
            pltpu.VMEM((8, wide), f32),
            pltpu.VMEM((8, wide), f32),
            pltpu.VMEM((8, wide), f32),
            pltpu.VMEM((8, wide), f32),
            pltpu.VMEM((8, zl * yl * LANES), f32),
            pltpu.VMEM((rounds, 8, LANES), f32),
            pltpu.VMEM((rounds, nslab, 8, LANES), f32),
            pltpu.VMEM((rounds, 8, LANES), f32),
            pltpu.VMEM((rounds, nsub, 8, LANES), f32),
            pltpu.VMEM((8, LANES), f32),
            pltpu.VMEM((8 * ITERS, LANES), f32),
            pltpu.VMEM((8 * ITERS, LANES), f32),
            dma((nsub,)),
            dma((nsub,)),
            dma((nsub,)),
            dma((nsub,)),
            dma((2,)),
            dma((2,)),
            dma((ITERS - 1, 2)),
            dma((ITERS - 1, 2)),
            dma((rounds, nslab)),
            dma((rounds, nslab)),
            dma((rounds, nsub)),
            dma((rounds, nsub)),
        ],
        compiler_params=pltpu.CompilerParams(
            collective_id=0, has_side_effects=True, vmem_limit_bytes=48 * 1024 * 1024
        ),
    )(rhs.reshape(-1, zs), perm.reshape(-1, zs), accum.reshape(-1, zs), counts)
    return out[0].reshape(rhs.shape), out[1].reshape(rhs.shape)


def choose(rhs, perm, accum, counts):
    nsub = lax.axis_size("sub")
    s, depth, cy, zs = rhs.shape
    nx = depth * nsub
    fits = s == S == nsub == 8 and zs == LANES and zs // nsub % 8 == 0 and LANES % nx == 0 and zs % nsub == 0 and zs // nsub > DEG
    fits = fits and cy % max(LANES // nx, 1) == 0 and cy // max(LANES // nx, 1) == 4
    if fits:
        return fast_body(rhs, perm, accum, counts)
    return body(rhs, perm, accum, counts)


def solution(mesh):
    placed = (P(None, "sub", None, "slab"), P("sub", None, "slab"), P("sub", None, "slab"), P())
    return jax.shard_map(
        choose,
        mesh=mesh,
        in_specs=placed,
        out_specs=(P(None, "sub", None, "slab"), P(None, "sub", None, "slab")),
        check_vma=False,
    )
```
